32 devices in a mesh: seq: 8 (over z, x), tp: 4 (over y, core).
Axes of the slice: x: 2, y: 2, z: 4, core: 2. Of those that a mesh axis runs over, the one named last changes fastest.
Arguments:
- tokens: bfloat16 [16384, 2560], P('seq'), may hold values from -6 to 6
- w_query: bfloat16 [2560, 512], P(None, 'tp'), may hold values from -0.009765625 to 0.009765625
- w_key: bfloat16 [2560, 512], P(None, 'tp'), may hold values from -0.0009765625 to 0.0009765625
- w_value: bfloat16 [2560, 1024], P(None, 'tp'), may hold values from -0.125 to 0.125
- w_gate: bfloat16 [2560, 512], P(None, 'tp'), may hold values from -0.125 to 0.125
- gate_rate: float32 [512], P('tp'), may hold values from 1.5258789e-05 to 0.00012207031
- out_grad: bfloat16 [16384, 1024], P('seq', 'tp'), may hold values from -6 to 6
Outputs:
- input_grad: bfloat16 [16384, 2560], P(('seq', 'tp'))
- gate_signal: float32 [16384, 512], P('seq', 'tp')
The draws below stay inside these ranges and needn't reach their ends.
All inputs are finite; a program needn't handle non-finite values.
Results may differ from the reference program's by a relative error of at most 0.015.
Values sent between devices are 32-bit elements.
A program may use at most 192 MiB of HBM per device.

```python
import math
import jax
import jax.numpy as jnp
from jax import lax

D = 2560
DK = 128
DV = 256
CH = 128
HEADS = 4
TOKENS = 16384


def block_levels(stream_key, extent, split, smallest, high):
    def one(dim, shards_of):
        heights = jax.random.uniform(jax.random.fold_in(jax.random.fold_in(stream_key, 6), dim), (shards_of,), jnp.float32, smallest / len(split), high / len(split))
        return jnp.repeat(jnp.exp(heights), extent[dim] // shards_of).reshape((-1,) + (1,) * (len(extent) - dim - 1))

    gain = one(*split[0])
    for cut in split[1:]:
        gain = gain * one(*cut)
    return gain


def centred(own_key, shape, scale, limit, shards=(), dtype=jnp.bfloat16):
    drawn = scale * jax.random.normal(own_key, shape, jnp.float32)
    if shards:
        drawn = drawn * block_levels(own_key, shape, shards, -0.22, 0.18)
    return jnp.clip(drawn, -limit, limit).astype(dtype)


def setup_inputs(seed: int = 0) -> dict:
    seeds = jax.random.split(jax.random.key(seed), 8)
    return {
        "tokens": centred(seeds[0], (TOKENS, D), 1.0, 6.0, ((0, 8),)),
        "w_query": centred(seeds[1], (D, HEADS * DK), (D * DK) ** -0.5, 0.009765625, ((1, 4),)),
        "w_key": centred(seeds[2], (D, HEADS * DK), (D * TOKENS) ** -0.5, 0.0009765625, ((1, 4),)),
        "w_value": centred(seeds[3], (D, HEADS * DV), D ** -0.5, 0.125, ((1, 4),)),
        "w_gate": centred(seeds[4], (D, HEADS * DK), D ** -0.5, 0.125, ((1, 4),)),
        "gate_rate": jnp.clip(jnp.exp(math.log(0.00012207031) - 2.0794415 * jax.random.uniform(seeds[5], (HEADS * DK,), jnp.float32) ** block_levels(seeds[5], (HEADS * DK,), ((0, 4),), -0.2, 0.2)), 1.52587890625e-05, 0.00012207031),
        "out_grad": centred(seeds[6], (TOKENS, HEADS * DV), 1.0, 6.0, ((0, 8), (1, 4))),
    }


def lower_ones(length):
    places = jnp.arange(length)
    return (places[:, None] >= places[None, :]).astype(jnp.float32)

def low_dot(left, right):
    return jnp.dot(left.astype(jnp.bfloat16), right.astype(jnp.bfloat16), preferred_element_type=jnp.float32)

def run_head(query_rows, key_rows, value_rows, log_gate, initial):
    block_size = CH
    blocks_count = query_rows.shape[0] // block_size
    triangle = lower_ones(block_size)
    pieces = tuple((a.reshape(blocks_count, block_size, a.shape[1]) for a in (query_rows, key_rows, value_rows, log_gate)))

    def advance(memory, piece):
        query_block, key_block, value_block, gate_block = piece
        within = jnp.cumsum(gate_block, axis=0)
        closing = within[-1]
        query_scaled = query_block * jnp.exp(within)
        key_scaled = key_block * jnp.exp(-within)
        scores = low_dot(query_scaled, key_scaled.T) * triangle
        output = low_dot(query_scaled, memory) + low_dot(scores, value_block)
        key_closing = key_block * jnp.exp(closing - within)
        memory = jnp.exp(closing)[:, None] * memory + low_dot(key_closing.T, value_block)
        return (memory, output)
    last_memory, outputs = lax.scan(advance, initial, pieces)
    return (outputs.reshape(-1, outputs.shape[2]), last_memory)

def by_heads(matrix, width):
    return matrix.astype(jnp.float32).reshape(matrix.shape[0], -1, width).transpose(1, 0, 2)

def by_tokens(stacked):
    return stacked.transpose(1, 0, 2).reshape(stacked.shape[1], -1)

def back_project(grad_rows, weight):
    return lax.dot_general(grad_rows, weight, (((1,), (1,)), ((), ())), preferred_element_type=jnp.float32)

def reference(tokens, w_query, w_key, w_value, w_gate, gate_rate, out_grad):
    queries = jnp.dot(tokens, w_query, preferred_element_type=jnp.float32).astype(jnp.bfloat16)
    keys_proj = jnp.dot(tokens, w_key, preferred_element_type=jnp.float32).astype(jnp.bfloat16)
    values_proj = jnp.dot(tokens, w_value, preferred_element_type=jnp.float32).astype(jnp.bfloat16)
    squashed = jax.nn.sigmoid(jnp.dot(tokens, w_gate, preferred_element_type=jnp.float32))
    log_gate = -gate_rate * squashed
    initial = jnp.zeros((HEADS, DK, DV), jnp.float32)

    def forward(query_heads, key_heads, value_heads, gate_heads):
        outputs, last_memory = jax.vmap(run_head)(query_heads, key_heads, value_heads, gate_heads, initial)
        return outputs
    outputs, pullback = jax.vjp(forward, by_heads(queries, DK), by_heads(keys_proj, DK), by_heads(values_proj, DV), by_heads(log_gate, DK))
    grads = pullback(by_heads(out_grad, DV))
    query_grad = by_tokens(grads[0]).astype(jnp.bfloat16)
    key_grad = by_tokens(grads[1]).astype(jnp.bfloat16)
    value_grad = by_tokens(grads[2]).astype(jnp.bfloat16)
    pre_grad = by_tokens(grads[3]) * -gate_rate * squashed * (1.0 - squashed)
    gate_signal = pre_grad * (4.0 * math.sqrt(TOKENS * DK / DV))
    gate_grad = pre_grad.astype(jnp.bfloat16)
    mixed = back_project(query_grad, w_query) + back_project(key_grad, w_key)
    mixed = mixed + back_project(value_grad, w_value) + back_project(gate_grad, w_gate)
    return (mixed.astype(jnp.bfloat16), gate_signal)
```

```python
import functools
import math

import jax
import jax.numpy as jnp
from jax import lax
from jax.experimental import pallas as pl
from jax.experimental.pallas import tpu as pltpu
from jax.sharding import PartitionSpec as P

CH = 128
PAD = 8
VMEM_LIMIT = 66 * 1000 * 1000
F32, BF16 = jnp.float32, jnp.bfloat16


def mm(left, right, dims):
    return lax.dot_general(left, right, (dims, ((), ())), preferred_element_type=F32)


NN = ((1,), (0,))
NT = ((1,), (1,))
TN = ((0,), (0,))


def tri_sum(triangle, rows):
    high = rows.astype(BF16)
    low = (rows - high.astype(F32)).astype(BF16)
    return mm(triangle, high, NN) + mm(triangle, low, NN)


def kernel(
    seq, tp, dk, dv, tile, scale,
    tok, wq, wk, wv, wg, rate_ref, dout_ref,
    grad_ref, sig_ref,
    wcat, xbuf, proj, sq_all, w_all, s_all, m_all, cl_all, msg, got, edge,
    send_a, recv_a, send_y, recv_y, send_b, recv_b,
    w_sem, x_sem, msg_send, msg_recv, sa_sem, ra_sem, sy_sem, ry_sem, sb_sem, rb_sem,
):
    me, rank = lax.axis_index("seq"), lax.axis_index("tp")
    length, width = dout_ref.shape[0], wcat.shape[0]
    blocks, tiles = length // CH, length // tile
    each = blocks // tp
    core = rank + 1 - 2 * lax.rem(rank, 2)
    far = lax.rem(rank + 2, 4)
    far_core = lax.rem(core + 2, 4)

    def x_copy(t, slot):
        return pltpu.make_async_copy(
            tok.at[pl.ds(pl.multiple_of(t * tile, tile), tile), :], xbuf.at[slot], x_sem.at[slot]
        )

    loads = []
    for n, (w, start, size) in enumerate(
        ((wq, 0, dk), (wk, dk, dk), (wv, 2 * dk, dv), (wg, 2 * dk + dv, dk))
    ):
        loads.append(pltpu.make_async_copy(w, wcat.at[:, pl.ds(start, size)], w_sem.at[n]))
    x_copy(0, 0).start()
    for load in loads:
        load.start()

    barrier = pltpu.get_barrier_semaphore()
    for d in range(1, seq):
        pl.semaphore_signal(
            barrier, inc=1, device_id={"seq": lax.rem(me + d, seq)},
            device_id_type=pl.DeviceIdType.MESH,
        )
    for other in (core, far):
        pl.semaphore_signal(
            barrier, inc=1, device_id={"tp": other}, device_id_type=pl.DeviceIdType.MESH
        )

    rows_at = lax.broadcasted_iota(jnp.int32, (CH, CH), 0)
    cols_at = lax.broadcasted_iota(jnp.int32, (CH, CH), 1)
    lower = (rows_at >= cols_at).astype(F32)
    lower_b = lower.astype(BF16)
    upper_b = (rows_at <= cols_at).astype(BF16)
    rate = rate_ref[...]

    zero_state = jnp.zeros((dv, dk), F32)
    msg[0, pl.ds(0, dv), :] = zero_state
    msg[1, pl.ds(0, dv), :] = zero_state
    for load in loads:
        load.wait()

    def project(t, total):
        slot = lax.rem(t, 2)

        @pl.when(t + 1 < tiles)
        def _():
            x_copy(t + 1, 1 - slot).start()

        x_copy(t, slot).wait()
        out = mm(xbuf[slot], wcat[...], NN)
        base = pl.multiple_of(t * tile, tile)
        proj[pl.ds(base, tile), :] = out[:, : 2 * dk + dv].astype(BF16)
        squashed = jax.nn.sigmoid(out[:, 2 * dk + dv :])
        sq_all[pl.ds(base, tile), :] = squashed
        for j in range(tile // CH):
            part = slice(j * CH, (j + 1) * CH)
            b = t * (tile // CH) + j
            within = tri_sum(lower_b, -rate * squashed[part])
            w_all[pl.ds(pl.multiple_of(base + j * CH, CH), CH), :] = within
            closing = within[CH - 1 : CH]
            cl_all[b] = jnp.broadcast_to(closing, (PAD, dk))
            query = out[part, :dk].astype(BF16).astype(F32)
            key = out[part, dk : 2 * dk].astype(BF16).astype(F32)
            value = out[part, 2 * dk : 2 * dk + dv].astype(BF16)
            dout = dout_ref[pl.ds(pl.multiple_of(base + j * CH, CH), CH), :]
            query_scaled = (query * jnp.exp(within)).astype(BF16)
            key_closing = (key * jnp.exp(closing - within)).astype(BF16)
            state = msg[0, pl.ds(0, dv), :]
            s_all[b] = state
            msg[0, pl.ds(0, dv), :] = jnp.exp(closing) * state + mm(value, key_closing, TN)
            fed = mm(dout, query_scaled, TN)
            m_all[b] = fed
            msg[1, pl.ds(0, dv), :] += jnp.exp(total) * fed
            total = total + closing
        return total

    total = lax.fori_loop(0, tiles, project, jnp.zeros((1, dk), F32))
    decay = jnp.broadcast_to(jnp.exp(total), (PAD, dk))
    msg[0, pl.ds(dv, PAD), :] = decay
    msg[1, pl.ds(dv, PAD), :] = decay

    pl.semaphore_wait(barrier, seq + 1)

    def exchange(d):
        return pltpu.make_async_remote_copy(
            src_ref=msg.at[(me + d) // seq],
            dst_ref=got.at[d],
            send_sem=msg_send.at[d],
            recv_sem=msg_recv.at[d],
            device_id={"seq": lax.rem(me + d, seq)},
            device_id_type=pl.DeviceIdType.MESH,
        )

    def start_exchange(d, carry):
        exchange(d).start()
        return carry

    def wait_exchange(d, carry):
        exchange(d).wait()
        return carry

    lax.fori_loop(1, seq, start_exchange, 0)
    lax.fori_loop(1, seq, wait_exchange, 0)

    edge[...] = jnp.zeros_like(edge)

    def fold(which, d):
        edge[which] = got[d, pl.ds(dv, 1), :] * edge[which] + got[d, pl.ds(0, dv), :]

    def fold_states(j, carry):
        fold(0, me - j)
        return carry

    def fold_grads(d, carry):
        fold(1, d)
        return carry

    lax.fori_loop(0, me, fold_states, 0)
    lax.fori_loop(me + 1, seq, fold_grads, 0)

    def enter(b, so_far):
        s_all[b] = s_all[b] + jnp.exp(so_far) * edge[0]
        return so_far + cl_all[b, 0:1, :]

    lax.fori_loop(0, blocks, enter, jnp.zeros((1, dk), F32))

    def leave(j, carry):
        b = blocks - 1 - j
        fed = m_all[b]
        leaving = edge[1]
        m_all[b] = leaving
        edge[1] = jnp.exp(cl_all[b, 0:1, :]) * leaving + fed
        return carry

    lax.fori_loop(0, blocks, leave, 0)

    def grads(b):
        rows = pl.ds(pl.multiple_of(b * CH, CH), CH)
        query = proj[rows, 0:dk].astype(F32)
        key = proj[rows, dk : 2 * dk].astype(F32)
        value = proj[rows, 2 * dk : 2 * dk + dv]
        within, squashed, dout = w_all[rows, :], sq_all[rows, :], dout_ref[rows, :]
        closing = within[CH - 1 : CH]
        state, leaving = s_all[b], m_all[b]
        grow, shrink, rest = jnp.exp(within), jnp.exp(-within), jnp.exp(closing - within)
        query_f, key_f, close_f = query * grow, key * shrink, key * rest
        query_s, key_s, close_s = query_f.astype(BF16), key_f.astype(BF16), close_f.astype(BF16)
        scores = (mm(query_s, key_s, NT) * lower).astype(BF16)
        d_scores = (mm(dout, value, NT) * lower).astype(BF16)
        leaving_b = leaving.astype(BF16)
        d_query_s = mm(dout, state.astype(BF16), NN) + mm(d_scores, key_s, NN)
        d_key_s = mm(d_scores, query_s, TN)
        d_close = mm(value, leaving_b, NN)
        d_value = mm(scores, dout, TN) + mm(close_s, leaving_b, NT)
        d_query = d_query_s * grow
        d_key = d_key_s * shrink + d_close * rest
        at_close = d_close * close_f
        d_within = d_query_s * query_f - d_key_s * key_f - at_close
        d_closing = jnp.sum(at_close, axis=0, keepdims=True) + jnp.exp(closing) * jnp.sum(
            leaving * state, axis=0, keepdims=True
        )
        d_gate = tri_sum(upper_b, d_within) + d_closing
        pre = d_gate * -rate * squashed * (1.0 - squashed)
        sig_ref[rows, :] = pre * scale
        return jnp.concatenate(
            [d_query.astype(BF16), d_key.astype(BF16), d_value.astype(BF16), pre.astype(BF16)],
            axis=1,
        )

    step = 512 if width % 512 == 0 else width

    def spread(packed, put):
        for at in range(0, width, step):
            cols = slice(at, at + step)
            put(cols, mm(packed, wcat[cols, :], NT))

    def remote(src, dst, sent, came, i, other):
        return pltpu.make_async_remote_copy(
            src_ref=src.at[i], dst_ref=dst.at[i], send_sem=sent.at[i], recv_sem=came.at[i],
            device_id={"tp": other}, device_id_type=pl.DeviceIdType.MESH,
        )

    def copy_a(i):
        return remote(send_a, recv_a, sa_sem, ra_sem, i, core)

    def copy_y(i):
        return remote(send_y, recv_y, sy_sem, ry_sem, i, far)

    def copy_b(i):
        return remote(send_b, recv_b, sb_sem, rb_sem, i, core)

    def away(i, carry):
        packed = grads(far_core * each + i)

        def put_a(cols, part):
            send_a[i, :, cols] = part

        spread(packed, put_a)
        copy_a(i).start()
        packed = grads(far * each + i)
        copy_a(i).wait()

        def put_y(cols, part):
            send_y[i, :, cols] = part + recv_a[i, :, cols]

        spread(packed, put_y)
        copy_y(i).start()
        return carry

    lax.fori_loop(0, each, away, 0)

    def home(i, carry):
        packed = grads(core * each + i)

        def put_b(cols, part):
            send_b[i, :, cols] = part

        spread(packed, put_b)
        copy_b(i).start()
        packed = grads(rank * each + i)
        copy_b(i).wait()

        def put_own(cols, part):
            send_a[i, :, cols] = part + recv_b[i, :, cols]

        spread(packed, put_own)
        return carry

    lax.fori_loop(0, each, home, 0)

    def finish(i, carry):
        copy_y(i).wait()
        rows = pl.ds(pl.multiple_of(i * CH, CH), CH)
        grad_ref[rows, :] = (send_a[i] + recv_y[i]).astype(BF16)
        return carry

    lax.fori_loop(0, each, finish, 0)


def solution(mesh):
    seq, tp = mesh.shape["seq"], mesh.shape["tp"]

    def body(tokens, w_query, w_key, w_value, w_gate, gate_rate, out_grad):
        length, width = tokens.shape
        dk, dv = w_query.shape[1], w_value.shape[1]
        blocks, each = length // CH, length // CH // tp
        tile = 2 * CH
        scale = 4.0 * math.sqrt(length * seq * dk / dv)
        piece = (each, CH, width)
        hbm = pl.BlockSpec(memory_space=pl.ANY)
        vmem = pl.BlockSpec(memory_space=pltpu.VMEM)
        dma = pltpu.SemaphoreType.DMA
        return pl.pallas_call(
            functools.partial(kernel, seq, tp, dk, dv, tile, scale),
            out_shape=(
                jax.ShapeDtypeStruct((length // tp, width), BF16),
                jax.ShapeDtypeStruct((length, dk), F32),
            ),
            in_specs=[hbm] * 5 + [vmem] * 2,
            out_specs=(vmem, vmem),
            scratch_shapes=[
                pltpu.VMEM((width, 3 * dk + dv), BF16),
                pltpu.VMEM((2, tile, width), BF16),
                pltpu.VMEM((length, 2 * dk + dv), BF16),
                pltpu.VMEM((length, dk), F32),
                pltpu.VMEM((length, dk), F32),
                pltpu.VMEM((blocks, dv, dk), F32),
                pltpu.VMEM((blocks, dv, dk), F32),
                pltpu.VMEM((blocks, PAD, dk), F32),
                pltpu.VMEM((2, dv + PAD, dk), F32),
                pltpu.VMEM((seq, dv + PAD, dk), F32),
                pltpu.VMEM((2, dv, dk), F32),
            ]
            + [pltpu.VMEM(piece, F32)] * 6
            + [dma((4,)), dma((2,)), dma((seq,)), dma((seq,))]
            + [dma((each,))] * 6,
            compiler_params=pltpu.CompilerParams(
                collective_id=0, has_side_effects=True, vmem_limit_bytes=VMEM_LIMIT
            ),
        )(tokens, w_query, w_key, w_value, w_gate, gate_rate.reshape(1, dk), out_grad)

    placed = (
        P("seq", None),
        P(None, "tp"),
        P(None, "tp"),
        P(None, "tp"),
        P(None, "tp"),
        P("tp"),
        P("seq", "tp"),
    )
    return jax.shard_map(
        body,
        mesh=mesh,
        in_specs=placed,
        out_specs=(P(("seq", "tp"), None), P("seq", "tp")),
        check_vma=False,
    )
```

```python
import functools
import math

import jax
import jax.numpy as jnp
from jax import lax
from jax.experimental import pallas as pl
from jax.experimental.pallas import tpu as pltpu
from jax.sharding import PartitionSpec as P

CH = 128
PAD = 8
VMEM_LIMIT = 66 * 1000 * 1000
F32, BF16 = jnp.float32, jnp.bfloat16


def mm(left, right, dims):
    return lax.dot_general(left, right, (dims, ((), ())), preferred_element_type=F32)


NN = ((1,), (0,))
NT = ((1,), (1,))
TN = ((0,), (0,))


def tri_sum(triangle, rows):
    high = rows.astype(BF16)
    low = (rows - high.astype(F32)).astype(BF16)
    return mm(triangle, high, NN) + mm(triangle, low, NN)


def kernel(
    seq, tp, dk, dv, tile, scale,
    tok, wq, wk, wv, wg, rate_ref, dout_ref,
    grad_ref, sig_ref,
    wcat, xbuf, proj, sq_all, w_all, s_all, m_all, cl_all, msg, got, edge,
    wout0, wout1, land0, land1, wfar, g_own, g_send, g_recv, part_own, part_send, part_recv,
    w_sem, x_sem, msg_send, msg_recv, gs_sem, gr_sem, ps_sem, pr_sem, first_sem, ring_s, ring_r,
):
    me, rank = lax.axis_index("seq"), lax.axis_index("tp")
    length, width = dout_ref.shape[0], wcat.shape[0]
    blocks, tiles = length // CH, length // tile
    each = blocks // tp
    core = rank + 1 - 2 * lax.rem(rank, 2)
    far = lax.rem(rank + 2, 4)
    far_core = lax.rem(core + 2, 4)
    half_ring, row = seq // 2, me // 2
    place = row + lax.rem(me, 2) * (seq - 1 - 2 * row)
    depth = width // seq

    def seq_at(p):
        p = lax.rem(p + seq, seq)
        return 2 * p + (p // half_ring) * (2 * seq - 1 - 4 * p)

    onward = (seq_at(place + 1), seq_at(place - 1))
    wouts, lands = (wout0, wout1), (land0, land1)
    starts = (0, wout0.shape[0])

    def cross(way):
        return pltpu.make_async_remote_copy(
            src_ref=wouts[way], dst_ref=lands[way].at[0], send_sem=first_sem.at[way],
            recv_sem=ring_r.at[way, 0], device_id={"tp": far},
            device_id_type=pl.DeviceIdType.MESH,
        )

    def ring(way, k):
        return pltpu.make_async_remote_copy(
            src_ref=lands[way].at[k], dst_ref=lands[way].at[k + 1], send_sem=ring_s.at[way, k],
            recv_sem=ring_r.at[way, k + 1], device_id={"seq": onward[way]},
            device_id_type=pl.DeviceIdType.MESH,
        )

    def pump(k):
        for way in (0, 1):
            if isinstance(k, int) and k == 0:
                cross(way).wait_recv()
            else:
                ring(way, k - 1).wait_recv()
            ring(way, k).start()

    def x_copy(t, slot):
        return pltpu.make_async_copy(
            tok.at[pl.ds(pl.multiple_of(t * tile, tile), tile), :], xbuf.at[slot], x_sem.at[slot]
        )

    loads = []
    for n, (w, start, size) in enumerate(
        ((wq, 0, dk), (wk, dk, dk), (wv, 2 * dk, dv), (wg, 2 * dk + dv, dk))
    ):
        loads.append(pltpu.make_async_copy(w, wcat.at[:, pl.ds(start, size)], w_sem.at[n]))
    x_copy(0, 0).start()
    for load in loads:
        load.start()

    barrier = pltpu.get_barrier_semaphore()
    for d in range(1, seq):
        pl.semaphore_signal(
            barrier, inc=1, device_id={"seq": lax.rem(me + d, seq)},
            device_id_type=pl.DeviceIdType.MESH,
        )
    for other in (core, far):
        pl.semaphore_signal(
            barrier, inc=1, device_id={"tp": other}, device_id_type=pl.DeviceIdType.MESH
        )

    rows_at = lax.broadcasted_iota(jnp.int32, (CH, CH), 0)
    cols_at = lax.broadcasted_iota(jnp.int32, (CH, CH), 1)
    lower = (rows_at >= cols_at).astype(F32)
    lower_b = lower.astype(BF16)
    upper_b = (rows_at <= cols_at).astype(BF16)
    rate = rate_ref[...]

    zero_state = jnp.zeros((dv, dk), F32)
    msg[0, pl.ds(0, dv), :] = zero_state
    msg[1, pl.ds(0, dv), :] = zero_state
    for load in loads:
        load.wait()
    for way in (0, 1):
        size = wouts[way].shape[0]
        at = pl.multiple_of(me * depth + starts[way], 16)
        wouts[way][...] = wcat[pl.ds(at, size), :].astype(F32)
    pl.semaphore_wait(barrier, seq + 1)
    for way in (0, 1):
        cross(way).start()

    def project(t, total):
        slot = lax.rem(t, 2)

        @pl.when(t + 1 < tiles)
        def _():
            x_copy(t + 1, 1 - slot).start()

        x_copy(t, slot).wait()
        out = mm(xbuf[slot], wcat[...], NN)
        base = pl.multiple_of(t * tile, tile)
        proj[pl.ds(base, tile), :] = out[:, : 2 * dk + dv].astype(BF16)
        squashed = jax.nn.sigmoid(out[:, 2 * dk + dv :])
        sq_all[pl.ds(base, tile), :] = squashed
        for j in range(tile // CH):
            part = slice(j * CH, (j + 1) * CH)
            b = t * (tile // CH) + j
            within = tri_sum(lower_b, -rate * squashed[part])
            w_all[pl.ds(pl.multiple_of(base + j * CH, CH), CH), :] = within
            closing = within[CH - 1 : CH]
            cl_all[b] = jnp.broadcast_to(closing, (PAD, dk))
            query = out[part, :dk].astype(BF16).astype(F32)
            key = out[part, dk : 2 * dk].astype(BF16).astype(F32)
            value = out[part, 2 * dk : 2 * dk + dv].astype(BF16)
            dout = dout_ref[pl.ds(pl.multiple_of(base + j * CH, CH), CH), :]
            query_scaled = (query * jnp.exp(within)).astype(BF16)
            key_closing = (key * jnp.exp(closing - within)).astype(BF16)
            state = msg[0, pl.ds(0, dv), :]
            s_all[b] = state
            msg[0, pl.ds(0, dv), :] = jnp.exp(closing) * state + mm(value, key_closing, TN)
            fed = mm(dout, query_scaled, TN)
            m_all[b] = fed
            msg[1, pl.ds(0, dv), :] += jnp.exp(total) * fed
            total = total + closing
        return total

    total = lax.fori_loop(0, tiles, project, jnp.zeros((1, dk), F32))
    decay = jnp.broadcast_to(jnp.exp(total), (PAD, dk))
    msg[0, pl.ds(dv, PAD), :] = decay
    msg[1, pl.ds(dv, PAD), :] = decay

    def exchange(d):
        return pltpu.make_async_remote_copy(
            src_ref=msg.at[(me + d) // seq],
            dst_ref=got.at[d],
            send_sem=msg_send.at[d],
            recv_sem=msg_recv.at[d],
            device_id={"seq": lax.rem(me + d, seq)},
            device_id_type=pl.DeviceIdType.MESH,
        )

    def start_exchange(d, carry):
        exchange(d).start()
        return carry

    def wait_exchange(d, carry):
        exchange(d).wait()
        return carry

    lax.fori_loop(1, seq, start_exchange, 0)
    pump(0)
    lax.fori_loop(1, seq, wait_exchange, 0)
    pump(1)

    edge[...] = jnp.zeros_like(edge)

    def fold(which, d):
        edge[which] = got[d, pl.ds(dv, 1), :] * edge[which] + got[d, pl.ds(0, dv), :]

    def fold_states(j, carry):
        fold(0, me - j)
        return carry

    def fold_grads(d, carry):
        fold(1, d)
        return carry

    lax.fori_loop(0, me, fold_states, 0)
    lax.fori_loop(me + 1, seq, fold_grads, 0)

    def enter(b, so_far):
        s_all[b] = s_all[b] + jnp.exp(so_far) * edge[0]
        return so_far + cl_all[b, 0:1, :]

    lax.fori_loop(0, blocks, enter, jnp.zeros((1, dk), F32))

    def leave(j, carry):
        b = blocks - 1 - j
        fed = m_all[b]
        leaving = edge[1]
        m_all[b] = leaving
        edge[1] = jnp.exp(cl_all[b, 0:1, :]) * leaving + fed
        return carry

    lax.fori_loop(0, blocks, leave, 0)

    def grads(b):
        rows = pl.ds(pl.multiple_of(b * CH, CH), CH)
        query = proj[rows, 0:dk].astype(F32)
        key = proj[rows, dk : 2 * dk].astype(F32)
        value = proj[rows, 2 * dk : 2 * dk + dv]
        within, squashed, dout = w_all[rows, :], sq_all[rows, :], dout_ref[rows, :]
        closing = within[CH - 1 : CH]
        state, leaving = s_all[b], m_all[b]
        grow, shrink, rest = jnp.exp(within), jnp.exp(-within), jnp.exp(closing - within)
        query_f, key_f, close_f = query * grow, key * shrink, key * rest
        query_s, key_s, close_s = query_f.astype(BF16), key_f.astype(BF16), close_f.astype(BF16)
        scores = (mm(query_s, key_s, NT) * lower).astype(BF16)
        d_scores = (mm(dout, value, NT) * lower).astype(BF16)
        leaving_b = leaving.astype(BF16)
        d_query_s = mm(dout, state.astype(BF16), NN) + mm(d_scores, key_s, NN)
        d_key_s = mm(d_scores, query_s, TN)
        d_close = mm(value, leaving_b, NN)
        d_value = mm(scores, dout, TN) + mm(close_s, leaving_b, NT)
        d_query = d_query_s * grow
        d_key = d_key_s * shrink + d_close * rest
        at_close = d_close * close_f
        d_within = d_query_s * query_f - d_key_s * key_f - at_close
        d_closing = jnp.sum(at_close, axis=0, keepdims=True) + jnp.exp(closing) * jnp.sum(
            leaving * state, axis=0, keepdims=True
        )
        d_gate = tri_sum(upper_b, d_within) + d_closing
        pre = d_gate * -rate * squashed * (1.0 - squashed)
        sig_ref[rows, :] = pre * scale
        return d_query, d_key, d_value, pre

    bounds = ((0, dk), (dk, 2 * dk), (2 * dk, 2 * dk + dv), (2 * dk + dv, 3 * dk + dv))
    step = 512 if width % 512 == 0 else width

    def spread(packed, weight, put):
        for at in range(0, width, step):
            cols = slice(at, at + step)
            put(cols, mm(packed, weight[cols, :], NT))

    def copy_g(i):
        return pltpu.make_async_remote_copy(
            src_ref=g_send.at[i], dst_ref=g_recv.at[i], send_sem=gs_sem.at[i],
            recv_sem=gr_sem.at[i], device_id={"tp": far}, device_id_type=pl.DeviceIdType.MESH,
        )

    def copy_p(i):
        return pltpu.make_async_remote_copy(
            src_ref=part_send.at[i], dst_ref=part_recv.at[i], send_sem=ps_sem.at[i],
            recv_sem=pr_sem.at[i], device_id={"tp": core}, device_id_type=pl.DeviceIdType.MESH,
        )

    def away(chunk, base):
        def run(i, carry):
            for (lo, hi), part in zip(bounds, grads(chunk * each + i)):
                g_send[base + i, :, lo:hi] = part
            copy_g(base + i).start()
            return carry

        lax.fori_loop(0, each, run, 0)

    def home(chunk, base):
        def run(i, carry):
            for (lo, hi), part in zip(bounds, grads(chunk * each + i)):
                g_own[base + i, :, lo:hi] = part.astype(BF16)
            return carry

        lax.fori_loop(0, each, run, 0)

    steps = iter(range(2, seq - 1))

    def pump_next():
        k = next(steps, None)
        if k is not None:
            pump(k)

    def rows_of(buffer, i):
        return jnp.concatenate([buffer[2 * i], buffer[2 * i + 1]], axis=0).astype(BF16)

    half = each // 2

    away(far_core, 0)
    pump_next()
    away(far, each)
    pump_next()
    home(core, 0)
    pump_next()
    home(rank, each)
    pump_next()

    def own_part(i, carry):
        def put_send(cols, part):
            part_send[i, :, cols] = part

        def put_own(cols, part):
            part_own[i, :, cols] = part

        spread(rows_of(g_own, i), wcat, put_send)
        spread(rows_of(g_own, half + i), wcat, put_own)
        return carry

    lax.fori_loop(0, half, own_part, 0)
    done = next(steps, seq - 1)

    def pump_rest(k, carry):
        pump(k)
        return carry

    lax.fori_loop(done, seq - 1, pump_rest, 0)
    for way in (0, 1):
        ring(way, seq - 2).wait_recv()

    def unpack(k, carry):
        for way in (0, 1):
            origin = seq_at(place + k) if way else seq_at(place - k)
            size = wouts[way].shape[0]
            at = pl.multiple_of(origin * depth + starts[way], 16)
            wfar[pl.ds(at, size), :] = lands[way][k].astype(BF16)
        return carry

    lax.fori_loop(0, seq, unpack, 0)

    def send_part(i, carry):
        copy_g(2 * i).wait()
        copy_g(2 * i + 1).wait()

        def put(cols, part):
            part_send[i, :, cols] = part_send[i, :, cols] + part

        spread(rows_of(g_recv, i), wfar, put)
        copy_p(i).start()
        return carry

    lax.fori_loop(0, half, send_part, 0)

    def finish(i, carry):
        copy_g(2 * (half + i)).wait()
        copy_g(2 * (half + i) + 1).wait()
        copy_p(i).wait()
        rows = pl.ds(pl.multiple_of(i * 2 * CH, 2 * CH), 2 * CH)

        def put(cols, part):
            grad_ref[rows, cols] = (
                part_own[i, :, cols] + part + part_recv[i, :, cols]
            ).astype(BF16)

        spread(rows_of(g_recv, half + i), wfar, put)
        return carry

    lax.fori_loop(0, half, finish, 0)

    def drain(k, carry):
        for way in (0, 1):
            ring(way, k).wait_send()
        return carry

    for way in (0, 1):
        cross(way).wait_send()
    lax.fori_loop(0, seq - 1, drain, 0)


def solution(mesh):
    seq, tp = mesh.shape["seq"], mesh.shape["tp"]

    def body(tokens, w_query, w_key, w_value, w_gate, gate_rate, out_grad):
        length, width = tokens.shape
        dk, dv = w_query.shape[1], w_value.shape[1]
        blocks, each = length // CH, length // CH // tp
        tile = 2 * CH
        scale = 4.0 * math.sqrt(length * seq * dk / dv)
        depth = width // seq
        upper = (depth // 2 + 15) // 16 * 16
        sizes = (upper, depth - upper)
        hbm = pl.BlockSpec(memory_space=pl.ANY)
        vmem = pl.BlockSpec(memory_space=pltpu.VMEM)
        dma = pltpu.SemaphoreType.DMA
        return pl.pallas_call(
            functools.partial(kernel, seq, tp, dk, dv, tile, scale),
            out_shape=(
                jax.ShapeDtypeStruct((length // tp, width), BF16),
                jax.ShapeDtypeStruct((length, dk), F32),
            ),
            in_specs=[hbm] * 5 + [vmem] * 2,
            out_specs=(vmem, vmem),
            scratch_shapes=[
                pltpu.VMEM((width, 3 * dk + dv), BF16),
                pltpu.VMEM((2, tile, width), BF16),
                pltpu.VMEM((length, 2 * dk + dv), BF16),
                pltpu.VMEM((length, dk), F32),
                pltpu.VMEM((length, dk), F32),
                pltpu.VMEM((blocks, dv, dk), F32),
                pltpu.VMEM((blocks, dv, dk), F32),
                pltpu.VMEM((blocks, PAD, dk), F32),
                pltpu.VMEM((2, dv + PAD, dk), F32),
                pltpu.VMEM((seq, dv + PAD, dk), F32),
                pltpu.VMEM((2, dv, dk), F32),
            ]
            + [pltpu.VMEM((size, 3 * dk + dv), F32) for size in sizes]
            + [pltpu.VMEM((seq, size, 3 * dk + dv), F32) for size in sizes]
            + [pltpu.VMEM((width, 3 * dk + dv), BF16)]
            + [pltpu.VMEM((2 * each, CH, 3 * dk + dv), kind) for kind in (BF16, F32, F32)]
            + [pltpu.VMEM((each // 2, 2 * CH, width), F32)] * 3
            + [dma((4,)), dma((2,)), dma((seq,)), dma((seq,))]
            + [dma((2 * each,))] * 2
            + [dma((each // 2,))] * 2
            + [dma((2,)), dma((2, seq)), dma((2, seq))],
            compiler_params=pltpu.CompilerParams(
                collective_id=0, has_side_effects=True, vmem_limit_bytes=VMEM_LIMIT
            ),
        )(tokens, w_query, w_key, w_value, w_gate, gate_rate.reshape(1, dk), out_grad)

    placed = (
        P("seq", None),
        P(None, "tp"),
        P(None, "tp"),
        P(None, "tp"),
        P(None, "tp"),
        P("tp"),
        P("seq", "tp"),
    )
    return jax.shard_map(
        body,
        mesh=mesh,
        in_specs=placed,
        out_specs=(P(("seq", "tp"), None), P("seq", "tp")),
        check_vma=False,
    )
```

```python
import functools
import math

import jax
import jax.numpy as jnp
from jax import lax
from jax.experimental import pallas as pl
from jax.experimental.pallas import tpu as pltpu
from jax.sharding import PartitionSpec as P

CH = 128
PAD = 8
VMEM_LIMIT = 66 * 1000 * 1000
F32, BF16 = jnp.float32, jnp.bfloat16


def mm(left, right, dims):
    return lax.dot_general(left, right, (dims, ((), ())), preferred_element_type=F32)


NN = ((1,), (0,))
NT = ((1,), (1,))
TN = ((0,), (0,))


def tri_sum(triangle, rows):
    high = rows.astype(BF16)
    low = (rows - high.astype(F32)).astype(BF16)
    return mm(triangle, high, NN) + mm(triangle, low, NN)


def kernel(
    seq, tp, dk, dv, tile, scale,
    tok, wq, wk, wv, wg, rate_ref, dout_ref,
    grad_ref, sig_ref,
    wcat, xbuf, proj, sq_all, w_all, s_all, m_all, cl_all, msg, got, edge,
    wout0, wout1, wout2, wout3, land0, land1, land2, land3, wfar, g_own, g_send, g_recv, part_own, part_send, part_recv,
    w_sem, x_sem, msg_send, msg_recv, gs_sem, gr_sem, ps_sem, pr_sem, first_sem, ring_s, ring_r,
):
    me, rank = lax.axis_index("seq"), lax.axis_index("tp")
    length, width = dout_ref.shape[0], wcat.shape[0]
    blocks, tiles = length // CH, length // tile
    each = blocks // tp
    half = each // 2
    core = rank + 1 - 2 * lax.rem(rank, 2)
    far = lax.rem(rank + 2, 4)
    far_core = lax.rem(core + 2, 4)
    half_ring, row = seq // 2, me // 2
    place = row + lax.rem(me, 2) * (seq - 1 - 2 * row)
    depth = width // seq

    def seq_at(p):
        p = lax.rem(p + seq, seq)
        return 2 * p + (p // half_ring) * (2 * seq - 1 - 4 * p)

    onward = (seq_at(place + 1), seq_at(place - 1))
    wouts, lands = (wout0, wout1, wout2, wout3), (land0, land1, land2, land3)
    starts = [sum(w.shape[0] for w in wouts[:n]) for n in range(4)]

    def cross(way):
        return pltpu.make_async_remote_copy(
            src_ref=wouts[way], dst_ref=lands[way].at[0], send_sem=first_sem.at[way],
            recv_sem=ring_r.at[way, 0], device_id={"tp": far},
            device_id_type=pl.DeviceIdType.MESH,
        )

    def ring(way, k):
        return pltpu.make_async_remote_copy(
            src_ref=lands[way].at[k], dst_ref=lands[way].at[k + 1], send_sem=ring_s.at[way, k],
            recv_sem=ring_r.at[way, k + 1], device_id={"seq": onward[way % 2]},
            device_id_type=pl.DeviceIdType.MESH,
        )

    def pump(k, part):
        for way in (2 * part, 2 * part + 1):
            if isinstance(k, int) and k == 0:
                cross(way).wait_recv()
            else:
                ring(way, k - 1).wait_recv()
            ring(way, k).start()

    def x_copy(t, slot):
        return pltpu.make_async_copy(
            tok.at[pl.ds(pl.multiple_of(t * tile, tile), tile), :], xbuf.at[slot], x_sem.at[slot]
        )

    loads = []
    for n, (w, start, size) in enumerate(
        ((wq, 0, dk), (wk, dk, dk), (wv, 2 * dk, dv), (wg, 2 * dk + dv, dk))
    ):
        loads.append(pltpu.make_async_copy(w, wcat.at[:, pl.ds(start, size)], w_sem.at[n]))
    x_copy(0, 0).start()
    for load in loads:
        load.start()

    barrier = pltpu.get_barrier_semaphore()
    for d in range(1, seq):
        pl.semaphore_signal(
            barrier, inc=1, device_id={"seq": lax.rem(me + d, seq)},
            device_id_type=pl.DeviceIdType.MESH,
        )
    for other in (core, far):
        pl.semaphore_signal(
            barrier, inc=1, device_id={"tp": other}, device_id_type=pl.DeviceIdType.MESH
        )

    rows_at = lax.broadcasted_iota(jnp.int32, (CH, CH), 0)
    cols_at = lax.broadcasted_iota(jnp.int32, (CH, CH), 1)
    lower = (rows_at >= cols_at).astype(F32)
    lower_b = lower.astype(BF16)
    upper_b = (rows_at <= cols_at).astype(BF16)
    rate = rate_ref[...]

    zero_state = jnp.zeros((dv, dk), F32)
    msg[0, pl.ds(0, dv), :] = zero_state
    msg[1, pl.ds(0, dv), :] = zero_state
    for load in loads:
        load.wait()
    for way in range(4):
        size = wouts[way].shape[0]
        at = pl.multiple_of(me * depth + starts[way], 16)
        wouts[way][...] = wcat[pl.ds(at, size), :].astype(F32)
    pl.semaphore_wait(barrier, seq + 1)
    for way in range(4):
        cross(way).start()

    def project(t, total):
        slot = lax.rem(t, 2)

        @pl.when(t + 1 < tiles)
        def _():
            x_copy(t + 1, 1 - slot).start()

        @pl.when(t == tiles - 2)
        def _():
            pump(0, 0)

        x_copy(t, slot).wait()
        out = mm(xbuf[slot], wcat[...], NN)
        base = pl.multiple_of(t * tile, tile)
        proj[pl.ds(base, tile), :] = out[:, : 2 * dk + dv].astype(BF16)
        squashed = jax.nn.sigmoid(out[:, 2 * dk + dv :])
        sq_all[pl.ds(base, tile), :] = squashed
        for j in range(tile // CH):
            part = slice(j * CH, (j + 1) * CH)
            b = t * (tile // CH) + j
            within = tri_sum(lower_b, -rate * squashed[part])
            w_all[pl.ds(pl.multiple_of(base + j * CH, CH), CH), :] = within
            closing = within[CH - 1 : CH]
            cl_all[b] = jnp.broadcast_to(closing, (PAD, dk))
            query = out[part, :dk].astype(BF16).astype(F32)
            key = out[part, dk : 2 * dk].astype(BF16).astype(F32)
            value = out[part, 2 * dk : 2 * dk + dv].astype(BF16)
            dout = dout_ref[pl.ds(pl.multiple_of(base + j * CH, CH), CH), :]
            query_scaled = (query * jnp.exp(within)).astype(BF16)
            key_closing = (key * jnp.exp(closing - within)).astype(BF16)
            state = msg[0, pl.ds(0, dv), :]
            s_all[b] = state
            msg[0, pl.ds(0, dv), :] = jnp.exp(closing) * state + mm(value, key_closing, TN)
            fed = mm(dout, query_scaled, TN)
            m_all[b] = fed
            msg[1, pl.ds(0, dv), :] += jnp.exp(total) * fed
            total = total + closing
        return total

    total = lax.fori_loop(0, tiles, project, jnp.zeros((1, dk), F32))
    decay = jnp.broadcast_to(jnp.exp(total), (PAD, dk))
    msg[0, pl.ds(dv, PAD), :] = decay
    msg[1, pl.ds(dv, PAD), :] = decay

    def exchange(d):
        return pltpu.make_async_remote_copy(
            src_ref=msg.at[(me + d) // seq],
            dst_ref=got.at[d],
            send_sem=msg_send.at[d],
            recv_sem=msg_recv.at[d],
            device_id={"seq": lax.rem(me + d, seq)},
            device_id_type=pl.DeviceIdType.MESH,
        )

    def start_exchange(d, carry):
        exchange(d).start()
        return carry

    def wait_exchange(d, carry):
        exchange(d).wait()
        return carry

    lax.fori_loop(1, seq, start_exchange, 0)
    pump(0, 1)
    lax.fori_loop(1, seq, wait_exchange, 0)
    pump(1, 0)

    edge[...] = jnp.zeros_like(edge)

    def fold(which, d):
        edge[which] = got[d, pl.ds(dv, 1), :] * edge[which] + got[d, pl.ds(0, dv), :]

    def fold_states(j, carry):
        fold(0, me - j)
        return carry

    def fold_grads(d, carry):
        fold(1, d)
        return carry

    lax.fori_loop(0, me, fold_states, 0)
    lax.fori_loop(me + 1, seq, fold_grads, 0)

    def enter(b, so_far):
        s_all[b] = s_all[b] + jnp.exp(so_far) * edge[0]
        return so_far + cl_all[b, 0:1, :]

    lax.fori_loop(0, blocks, enter, jnp.zeros((1, dk), F32))

    def leave(j, carry):
        b = blocks - 1 - j
        fed = m_all[b]
        leaving = edge[1]
        m_all[b] = leaving
        edge[1] = jnp.exp(cl_all[b, 0:1, :]) * leaving + fed
        return carry

    lax.fori_loop(0, blocks, leave, 0)

    def grads(b):
        rows = pl.ds(pl.multiple_of(b * CH, CH), CH)
        query = proj[rows, 0:dk].astype(F32)
        key = proj[rows, dk : 2 * dk].astype(F32)
        value = proj[rows, 2 * dk : 2 * dk + dv]
        within, squashed, dout = w_all[rows, :], sq_all[rows, :], dout_ref[rows, :]
        closing = within[CH - 1 : CH]
        state, leaving = s_all[b], m_all[b]
        grow, shrink, rest = jnp.exp(within), jnp.exp(-within), jnp.exp(closing - within)
        query_f, key_f, close_f = query * grow, key * shrink, key * rest
        query_s, key_s, close_s = query_f.astype(BF16), key_f.astype(BF16), close_f.astype(BF16)
        scores = (mm(query_s, key_s, NT) * lower).astype(BF16)
        d_scores = (mm(dout, value, NT) * lower).astype(BF16)
        leaving_b = leaving.astype(BF16)
        d_query_s = mm(dout, state.astype(BF16), NN) + mm(d_scores, key_s, NN)
        d_key_s = mm(d_scores, query_s, TN)
        d_close = mm(value, leaving_b, NN)
        d_value = mm(scores, dout, TN) + mm(close_s, leaving_b, NT)
        d_query = d_query_s * grow
        d_key = d_key_s * shrink + d_close * rest
        at_close = d_close * close_f
        d_within = d_query_s * query_f - d_key_s * key_f - at_close
        d_closing = jnp.sum(at_close, axis=0, keepdims=True) + jnp.exp(closing) * jnp.sum(
            leaving * state, axis=0, keepdims=True
        )
        d_gate = tri_sum(upper_b, d_within) + d_closing
        pre = d_gate * -rate * squashed * (1.0 - squashed)
        sig_ref[rows, :] = pre * scale
        return d_query, d_key, d_value, pre

    bounds = ((0, dk), (dk, 2 * dk), (2 * dk, 2 * dk + dv), (2 * dk + dv, 3 * dk + dv))
    step = 512 if width % 512 == 0 else width

    def spread(packed, weight, put):
        for at in range(0, width, step):
            cols = slice(at, at + step)
            put(cols, mm(packed, weight[cols, :], NT))

    def copy_g(i):
        return pltpu.make_async_remote_copy(
            src_ref=g_send.at[i], dst_ref=g_recv.at[i], send_sem=gs_sem.at[i],
            recv_sem=gr_sem.at[i], device_id={"tp": far}, device_id_type=pl.DeviceIdType.MESH,
        )

    def copy_p(i):
        return pltpu.make_async_remote_copy(
            src_ref=part_send.at[i], dst_ref=part_recv.at[i], send_sem=ps_sem.at[i],
            recv_sem=pr_sem.at[i], device_id={"tp": core}, device_id_type=pl.DeviceIdType.MESH,
        )

    steps = iter([(k, part) for k in range(1, seq - 1) for part in (0, 1)][1:])

    def pump_next():
        k = next(steps, None)
        if k is not None:
            pump(*k)

    def away(chunk, base):
        def run(i, carry):
            for (lo, hi), part in zip(bounds, grads(chunk * each + i)):
                g_send[base + i, :, lo:hi] = part
            copy_g(base + i).start()
            return carry

        lax.fori_loop(0, half, run, 0)
        pump_next()
        lax.fori_loop(half, each, run, 0)
        pump_next()

    def home(chunk, base):
        def run(i, carry):
            for (lo, hi), part in zip(bounds, grads(chunk * each + i)):
                g_own[base + i, :, lo:hi] = part.astype(BF16)
            return carry

        lax.fori_loop(0, half, run, 0)
        pump_next()
        lax.fori_loop(half, each, run, 0)
        pump_next()

    def rows_of(buffer, i):
        return jnp.concatenate([buffer[2 * i], buffer[2 * i + 1]], axis=0).astype(BF16)

    away(far_core, 0)
    away(far, each)
    home(core, 0)
    home(rank, each)

    def own_part(i, carry):
        def put_send(cols, part):
            part_send[i, :, cols] = part

        def put_own(cols, part):
            part_own[i, :, cols] = part

        spread(rows_of(g_own, i), wcat, put_send)
        spread(rows_of(g_own, half + i), wcat, put_own)
        return carry

    lax.fori_loop(0, half, own_part, 0)
    done, part = next(steps, (seq - 1, 0))
    if part == 1:
        pump(done, 1)
        done += 1

    def pump_rest(k, carry):
        pump(k, 0)
        pump(k, 1)
        return carry

    lax.fori_loop(done, seq - 1, pump_rest, 0)
    for way in range(4):
        ring(way, seq - 2).wait_recv()

    def unpack(k, carry):
        for way in range(4):
            origin = seq_at(place + k) if way % 2 else seq_at(place - k)
            size = wouts[way].shape[0]
            at = pl.multiple_of(origin * depth + starts[way], 16)
            wfar[pl.ds(at, size), :] = lands[way][k].astype(BF16)
        return carry

    lax.fori_loop(0, seq, unpack, 0)

    def send_part(i, carry):
        copy_g(2 * i).wait()
        copy_g(2 * i + 1).wait()

        def put(cols, part):
            part_send[i, :, cols] = part_send[i, :, cols] + part

        spread(rows_of(g_recv, i), wfar, put)
        copy_p(i).start()
        return carry

    lax.fori_loop(0, half, send_part, 0)

    def finish(i, carry):
        copy_g(2 * (half + i)).wait()
        copy_g(2 * (half + i) + 1).wait()
        copy_p(i).wait()
        rows = pl.ds(pl.multiple_of(i * 2 * CH, 2 * CH), 2 * CH)

        def put(cols, part):
            grad_ref[rows, cols] = (
                part_own[i, :, cols] + part + part_recv[i, :, cols]
            ).astype(BF16)

        spread(rows_of(g_recv, half + i), wfar, put)
        return carry

    lax.fori_loop(0, half, finish, 0)

    def drain(k, carry):
        for way in range(4):
            ring(way, k).wait_send()
        return carry

    for way in range(4):
        cross(way).wait_send()
    lax.fori_loop(0, seq - 1, drain, 0)


def solution(mesh):
    seq, tp = mesh.shape["seq"], mesh.shape["tp"]

    def body(tokens, w_query, w_key, w_value, w_gate, gate_rate, out_grad):
        length, width = tokens.shape
        dk, dv = w_query.shape[1], w_value.shape[1]
        blocks, each = length // CH, length // CH // tp
        tile = 2 * CH
        scale = 4.0 * math.sqrt(length * seq * dk / dv)
        depth = width // seq
        units = depth // 16
        sizes = [16 * ((units + 3 - n) // 4) for n in range(4)]
        hbm = pl.BlockSpec(memory_space=pl.ANY)
        vmem = pl.BlockSpec(memory_space=pltpu.VMEM)
        dma = pltpu.SemaphoreType.DMA
        return pl.pallas_call(
            functools.partial(kernel, seq, tp, dk, dv, tile, scale),
            out_shape=(
                jax.ShapeDtypeStruct((length // tp, width), BF16),
                jax.ShapeDtypeStruct((length, dk), F32),
            ),
            in_specs=[hbm] * 5 + [vmem] * 2,
            out_specs=(vmem, vmem),
            scratch_shapes=[
                pltpu.VMEM((width, 3 * dk + dv), BF16),
                pltpu.VMEM((2, tile, width), BF16),
                pltpu.VMEM((length, 2 * dk + dv), BF16),
                pltpu.VMEM((length, dk), F32),
                pltpu.VMEM((length, dk), F32),
                pltpu.VMEM((blocks, dv, dk), F32),
                pltpu.VMEM((blocks, dv, dk), F32),
                pltpu.VMEM((blocks, PAD, dk), F32),
                pltpu.VMEM((2, dv + PAD, dk), F32),
                pltpu.VMEM((seq, dv + PAD, dk), F32),
                pltpu.VMEM((2, dv, dk), F32),
            ]
            + [pltpu.VMEM((size, 3 * dk + dv), F32) for size in sizes]
            + [pltpu.VMEM((seq, size, 3 * dk + dv), F32) for size in sizes]
            + [pltpu.VMEM((width, 3 * dk + dv), BF16)]
            + [pltpu.VMEM((2 * each, CH, 3 * dk + dv), kind) for kind in (BF16, F32, F32)]
            + [pltpu.VMEM((each // 2, 2 * CH, width), F32)] * 3
            + [dma((4,)), dma((2,)), dma((seq,)), dma((seq,))]
            + [dma((2 * each,))] * 2
            + [dma((each // 2,))] * 2
            + [dma((4,)), dma((4, seq)), dma((4, seq))],
            compiler_params=pltpu.CompilerParams(
                collective_id=0, has_side_effects=True, vmem_limit_bytes=VMEM_LIMIT
            ),
        )(tokens, w_query, w_key, w_value, w_gate, gate_rate.reshape(1, dk), out_grad)

    placed = (
        P("seq", None),
        P(None, "tp"),
        P(None, "tp"),
        P(None, "tp"),
        P(None, "tp"),
        P("tp"),
        P("seq", "tp"),
    )
    return jax.shard_map(
        body,
        mesh=mesh,
        in_specs=placed,
        out_specs=(P(("seq", "tp"), None), P("seq", "tp")),
        check_vma=False,
    )
```

```python
import functools
import math

import jax
import jax.numpy as jnp
from jax import lax
from jax.experimental import pallas as pl
from jax.experimental.pallas import tpu as pltpu
from jax.sharding import PartitionSpec as P

CH = 128
PAD = 8
VMEM_LIMIT = 66 * 1000 * 1000
F32, BF16 = jnp.float32, jnp.bfloat16


def mm(left, right, dims):
    return lax.dot_general(left, right, (dims, ((), ())), preferred_element_type=F32)


NN = ((1,), (0,))
NT = ((1,), (1,))
TN = ((0,), (0,))


def tri_sum(triangle, rows):
    high = rows.astype(BF16)
    low = (rows - high.astype(F32)).astype(BF16)
    return mm(triangle, high, NN) + mm(triangle, low, NN)


def kernel(
    seq, tp, dk, dv, tile, scale,
    tok, wq, wk, wv, wg, rate_ref, dout_ref,
    grad_ref, sig_ref,
    wcat, xbuf, proj, sq_all, w_all, s_all, m_all, cl_all, msg, got, edge,
    wout0, wout1, wout2, wout3, land0, land1, land2, land3, wfar, g_own, g_send, g_recv, part_own, part_send, part_recv,
    w_sem, x_sem, msg_send, msg_recv, gs_sem, gr_sem, ps_sem, pr_sem, first_sem, ring_s, ring_r,
):
    me, rank = lax.axis_index("seq"), lax.axis_index("tp")
    length, width = dout_ref.shape[0], wcat.shape[0]
    blocks, tiles = length // CH, length // tile
    each = blocks // tp
    half = each // 2
    core = rank + 1 - 2 * lax.rem(rank, 2)
    far = lax.rem(rank + 2, 4)
    far_core = lax.rem(core + 2, 4)
    half_ring, row = seq // 2, me // 2
    place = row + lax.rem(me, 2) * (seq - 1 - 2 * row)
    depth = width // seq

    def seq_at(p):
        p = lax.rem(p + seq, seq)
        return 2 * p + (p // half_ring) * (2 * seq - 1 - 4 * p)

    onward = (seq_at(place + 1), seq_at(place - 1))
    wouts, lands = (wout0, wout1, wout2, wout3), (land0, land1, land2, land3)
    starts = [sum(w.shape[0] for w in wouts[:n]) for n in range(4)]

    def cross(way):
        return pltpu.make_async_remote_copy(
            src_ref=wouts[way], dst_ref=lands[way].at[0], send_sem=first_sem.at[way],
            recv_sem=ring_r.at[way, 0], device_id={"tp": far},
            device_id_type=pl.DeviceIdType.MESH,
        )

    def ring(way, k):
        return pltpu.make_async_remote_copy(
            src_ref=lands[way].at[k], dst_ref=lands[way].at[k + 1], send_sem=ring_s.at[way, k],
            recv_sem=ring_r.at[way, k + 1], device_id={"seq": onward[way % 2]},
            device_id_type=pl.DeviceIdType.MESH,
        )

    def pump(k, part):
        for way in (2 * part, 2 * part + 1):
            if isinstance(k, int) and k == 0:
                cross(way).wait_recv()
            else:
                ring(way, k - 1).wait_recv()
            ring(way, k).start()

    def x_copy(t, slot):
        return pltpu.make_async_copy(
            tok.at[pl.ds(pl.multiple_of(t * tile, tile), tile), :], xbuf.at[slot], x_sem.at[slot]
        )

    loads = []
    for n, (w, start, size) in enumerate(
        ((wq, 0, dk), (wk, dk, dk), (wv, 2 * dk, dv), (wg, 2 * dk + dv, dk))
    ):
        loads.append(pltpu.make_async_copy(w, wcat.at[:, pl.ds(start, size)], w_sem.at[n]))
    x_copy(0, 0).start()
    for load in loads:
        load.start()

    barrier = pltpu.get_barrier_semaphore()
    for d in range(1, seq):
        pl.semaphore_signal(
            barrier, inc=1, device_id={"seq": lax.rem(me + d, seq)},
            device_id_type=pl.DeviceIdType.MESH,
        )
    for other in (core, far):
        pl.semaphore_signal(
            barrier, inc=1, device_id={"tp": other}, device_id_type=pl.DeviceIdType.MESH
        )

    rows_at = lax.broadcasted_iota(jnp.int32, (CH, CH), 0)
    cols_at = lax.broadcasted_iota(jnp.int32, (CH, CH), 1)
    lower = (rows_at >= cols_at).astype(F32)
    lower_b = lower.astype(BF16)
    upper_b = (rows_at <= cols_at).astype(BF16)
    rate = rate_ref[...]

    zero_state = jnp.zeros((dv, dk), F32)
    msg[0, pl.ds(0, dv), :] = zero_state
    msg[1, pl.ds(0, dv), :] = zero_state
    for load in loads:
        load.wait()
    for way in range(4):
        size = wouts[way].shape[0]
        at = pl.multiple_of(me * depth + starts[way], 16)
        wouts[way][...] = wcat[pl.ds(at, size), :].astype(F32)
    pl.semaphore_wait(barrier, seq + 1)
    for way in range(4):
        cross(way).start()

    def project(t, total):
        slot = lax.rem(t, 2)

        @pl.when(t + 1 < tiles)
        def _():
            x_copy(t + 1, 1 - slot).start()

        @pl.when(t == tiles - 2)
        def _():
            pump(0, 0)

        x_copy(t, slot).wait()
        out = mm(xbuf[slot], wcat[...], NN)
        base = pl.multiple_of(t * tile, tile)
        proj[pl.ds(base, tile), :] = out[:, : 2 * dk + dv].astype(BF16)
        squashed = jax.nn.sigmoid(out[:, 2 * dk + dv :])
        sq_all[pl.ds(base, tile), :] = squashed
        for j in range(tile // CH):
            part = slice(j * CH, (j + 1) * CH)
            b = t * (tile // CH) + j
            within = tri_sum(lower_b, -rate * squashed[part])
            w_all[pl.ds(pl.multiple_of(base + j * CH, CH), CH), :] = within
            closing = within[CH - 1 : CH]
            cl_all[b] = jnp.broadcast_to(closing, (PAD, dk))
            query = out[part, :dk].astype(BF16).astype(F32)
            key = out[part, dk : 2 * dk].astype(BF16).astype(F32)
            value = out[part, 2 * dk : 2 * dk + dv].astype(BF16)
            dout = dout_ref[pl.ds(pl.multiple_of(base + j * CH, CH), CH), :]
            query_scaled = (query * jnp.exp(within)).astype(BF16)
            key_closing = (key * jnp.exp(closing - within)).astype(BF16)
            state = msg[0, pl.ds(0, dv), :]
            s_all[b] = state
            msg[0, pl.ds(0, dv), :] = jnp.exp(closing) * state + mm(value, key_closing, TN)
            fed = mm(dout, query_scaled, TN)
            m_all[b] = fed
            msg[1, pl.ds(0, dv), :] += jnp.exp(total) * fed
            total = total + closing
        return total

    total = lax.fori_loop(0, tiles, project, jnp.zeros((1, dk), F32))
    decay = jnp.broadcast_to(jnp.exp(total), (PAD, dk))
    msg[0, pl.ds(dv, PAD), :] = decay
    msg[1, pl.ds(dv, PAD), :] = decay

    def exchange(d):
        return pltpu.make_async_remote_copy(
            src_ref=msg.at[(me + d) // seq],
            dst_ref=got.at[d],
            send_sem=msg_send.at[d],
            recv_sem=msg_recv.at[d],
            device_id={"seq": lax.rem(me + d, seq)},
            device_id_type=pl.DeviceIdType.MESH,
        )

    def start_exchange(d, carry):
        exchange(d).start()
        return carry

    def wait_exchange(d, carry):
        exchange(d).wait()
        return carry

    lax.fori_loop(1, seq, start_exchange, 0)
    pump(0, 1)
    lax.fori_loop(1, seq, wait_exchange, 0)
    pump(1, 0)

    edge[...] = jnp.zeros_like(edge)

    def fold(which, d):
        edge[which] = got[d, pl.ds(dv, 1), :] * edge[which] + got[d, pl.ds(0, dv), :]

    def fold_states(j, carry):
        fold(0, me - j)
        return carry

    def fold_grads(d, carry):
        fold(1, d)
        return carry

    lax.fori_loop(0, me, fold_states, 0)
    lax.fori_loop(me + 1, seq, fold_grads, 0)

    def enter(b, so_far):
        s_all[b] = s_all[b] + jnp.exp(so_far) * edge[0]
        return so_far + cl_all[b, 0:1, :]

    lax.fori_loop(0, blocks, enter, jnp.zeros((1, dk), F32))

    def leave(j, carry):
        b = blocks - 1 - j
        fed = m_all[b]
        leaving = edge[1]
        m_all[b] = leaving
        edge[1] = jnp.exp(cl_all[b, 0:1, :]) * leaving + fed
        return carry

    lax.fori_loop(0, blocks, leave, 0)

    def grads(b):
        rows = pl.ds(pl.multiple_of(b * CH, CH), CH)
        query = proj[rows, 0:dk].astype(F32)
        key = proj[rows, dk : 2 * dk].astype(F32)
        value = proj[rows, 2 * dk : 2 * dk + dv]
        within, squashed, dout = w_all[rows, :], sq_all[rows, :], dout_ref[rows, :]
        closing = within[CH - 1 : CH]
        state, leaving = s_all[b], m_all[b]
        grow, shrink, rest = jnp.exp(within), jnp.exp(-within), jnp.exp(closing - within)
        query_f, key_f, close_f = query * grow, key * shrink, key * rest
        query_s, key_s, close_s = query_f.astype(BF16), key_f.astype(BF16), close_f.astype(BF16)
        scores = (mm(query_s, key_s, NT) * lower).astype(BF16)
        d_scores = (mm(dout, value, NT) * lower).astype(BF16)
        leaving_b = leaving.astype(BF16)
        d_query_s = mm(dout, state.astype(BF16), NN) + mm(d_scores, key_s, NN)
        d_key_s = mm(d_scores, query_s, TN)
        d_close = mm(value, leaving_b, NN)
        d_value = mm(scores, dout, TN) + mm(close_s, leaving_b, NT)
        d_query = d_query_s * grow
        d_key = d_key_s * shrink + d_close * rest
        at_close = d_close * close_f
        d_within = d_query_s * query_f - d_key_s * key_f - at_close
        d_closing = jnp.sum(at_close, axis=0, keepdims=True) + jnp.exp(closing) * jnp.sum(
            leaving * state, axis=0, keepdims=True
        )
        d_gate = tri_sum(upper_b, d_within) + d_closing
        pre = d_gate * -rate * squashed * (1.0 - squashed)
        sig_ref[rows, :] = pre * scale
        return d_query, d_key, d_value, pre

    bounds = ((0, dk), (dk, 2 * dk), (2 * dk, 2 * dk + dv), (2 * dk + dv, 3 * dk + dv))
    step = 512 if width % 512 == 0 else width

    def spread(packed, weight, put):
        for at in range(0, width, step):
            cols = slice(at, at + step)
            put(cols, mm(packed, weight[cols, :], NT))

    def copy_g(i):
        return pltpu.make_async_remote_copy(
            src_ref=g_send.at[i], dst_ref=g_recv.at[i], send_sem=gs_sem.at[i],
            recv_sem=gr_sem.at[i], device_id={"tp": far}, device_id_type=pl.DeviceIdType.MESH,
        )

    def copy_p(i):
        return pltpu.make_async_remote_copy(
            src_ref=part_send.at[i], dst_ref=part_recv.at[i], send_sem=ps_sem.at[i],
            recv_sem=pr_sem.at[i], device_id={"tp": core}, device_id_type=pl.DeviceIdType.MESH,
        )

    steps = iter([(k, part) for k in range(1, seq - 1) for part in (0, 1)][1:])

    def pump_next():
        k = next(steps, None)
        if k is not None:
            pump(*k)

    def away(chunk, base):
        def run(i, carry):
            for (lo, hi), part in zip(bounds, grads(chunk * each + i)):
                g_send[base + i, :, lo:hi] = part
            copy_g(base + i).start()
            return carry

        lax.fori_loop(0, half, run, 0)
        pump_next()
        lax.fori_loop(half, each, run, 0)
        pump_next()

    def home(chunk, base):
        def run(i, carry):
            for (lo, hi), part in zip(bounds, grads(chunk * each + i)):
                g_own[base + i, :, lo:hi] = part.astype(BF16)
            return carry

        lax.fori_loop(0, half, run, 0)
        pump_next()
        lax.fori_loop(half, each, run, 0)
        pump_next()

    def rows_of(buffer, i):
        return jnp.concatenate([buffer[2 * i], buffer[2 * i + 1]], axis=0).astype(BF16)

    away(far_core, 0)
    away(far, each)
    home(core, 0)
    home(rank, each)

    def own_part(i, carry):
        def put_send(cols, part):
            part_send[i, :, cols] = part

        def put_own(cols, part):
            part_own[i, :, cols] = part

        spread(rows_of(g_own, i), wcat, put_send)
        spread(rows_of(g_own, half + i), wcat, put_own)
        return carry

    lax.fori_loop(0, half, own_part, 0)
    done, part = next(steps, (seq - 1, 0))
    if part == 1:
        pump(done, 1)
        done += 1

    def pump_rest(k, carry):
        pump(k, 0)
        pump(k, 1)
        return carry

    lax.fori_loop(done, seq - 1, pump_rest, 0)
    def unpack(k, carry):
        for way in range(4):
            origin = seq_at(place + k) if way % 2 else seq_at(place - k)
            size = wouts[way].shape[0]
            at = pl.multiple_of(origin * depth + starts[way], 16)
            wfar[pl.ds(at, size), :] = lands[way][k].astype(BF16)
        return carry

    lax.fori_loop(0, seq - 1, unpack, 0)
    for way in range(4):
        ring(way, seq - 2).wait_recv()
    unpack(seq - 1, 0)

    def send_part(i, carry):
        copy_g(2 * i).wait()
        copy_g(2 * i + 1).wait()

        def put(cols, part):
            part_send[i, :, cols] = part_send[i, :, cols] + part

        spread(rows_of(g_recv, i), wfar, put)
        copy_p(i).start()
        return carry

    lax.fori_loop(0, half, send_part, 0)

    def finish(i, carry):
        copy_g(2 * (half + i)).wait()
        copy_g(2 * (half + i) + 1).wait()
        copy_p(i).wait()
        rows = pl.ds(pl.multiple_of(i * 2 * CH, 2 * CH), 2 * CH)

        def put(cols, part):
            grad_ref[rows, cols] = (
                part_own[i, :, cols] + part + part_recv[i, :, cols]
            ).astype(BF16)

        spread(rows_of(g_recv, half + i), wfar, put)
        return carry

    lax.fori_loop(0, half, finish, 0)

    def drain(k, carry):
        for way in range(4):
            ring(way, k).wait_send()
        return carry

    for way in range(4):
        cross(way).wait_send()
    lax.fori_loop(0, seq - 1, drain, 0)


def solution(mesh):
    seq, tp = mesh.shape["seq"], mesh.shape["tp"]

    def body(tokens, w_query, w_key, w_value, w_gate, gate_rate, out_grad):
        length, width = tokens.shape
        dk, dv = w_query.shape[1], w_value.shape[1]
        blocks, each = length // CH, length // CH // tp
        tile = 2 * CH
        scale = 4.0 * math.sqrt(length * seq * dk / dv)
        depth = width // seq
        units = depth // 16
        sizes = [16 * ((units + 3 - n) // 4) for n in range(4)]
        hbm = pl.BlockSpec(memory_space=pl.ANY)
        vmem = pl.BlockSpec(memory_space=pltpu.VMEM)
        dma = pltpu.SemaphoreType.DMA
        return pl.pallas_call(
            functools.partial(kernel, seq, tp, dk, dv, tile, scale),
            out_shape=(
                jax.ShapeDtypeStruct((length // tp, width), BF16),
                jax.ShapeDtypeStruct((length, dk), F32),
            ),
            in_specs=[hbm] * 5 + [vmem] * 2,
            out_specs=(vmem, vmem),
            scratch_shapes=[
                pltpu.VMEM((width, 3 * dk + dv), BF16),
                pltpu.VMEM((2, tile, width), BF16),
                pltpu.VMEM((length, 2 * dk + dv), BF16),
                pltpu.VMEM((length, dk), F32),
                pltpu.VMEM((length, dk), F32),
                pltpu.VMEM((blocks, dv, dk), F32),
                pltpu.VMEM((blocks, dv, dk), F32),
                pltpu.VMEM((blocks, PAD, dk), F32),
                pltpu.VMEM((2, dv + PAD, dk), F32),
                pltpu.VMEM((seq, dv + PAD, dk), F32),
                pltpu.VMEM((2, dv, dk), F32),
            ]
            + [pltpu.VMEM((size, 3 * dk + dv), F32) for size in sizes]
            + [pltpu.VMEM((seq, size, 3 * dk + dv), F32) for size in sizes]
            + [pltpu.VMEM((width, 3 * dk + dv), BF16)]
            + [pltpu.VMEM((2 * each, CH, 3 * dk + dv), kind) for kind in (BF16, F32, F32)]
            + [pltpu.VMEM((each // 2, 2 * CH, width), F32)] * 3
            + [dma((4,)), dma((2,)), dma((seq,)), dma((seq,))]
            + [dma((2 * each,))] * 2
            + [dma((each // 2,))] * 2
            + [dma((4,)), dma((4, seq)), dma((4, seq))],
            compiler_params=pltpu.CompilerParams(
                collective_id=0, has_side_effects=True, vmem_limit_bytes=VMEM_LIMIT
            ),
        )(tokens, w_query, w_key, w_value, w_gate, gate_rate.reshape(1, dk), out_grad)

    placed = (
        P("seq", None),
        P(None, "tp"),
        P(None, "tp"),
        P(None, "tp"),
        P(None, "tp"),
        P("tp"),
        P("seq", "tp"),
    )
    return jax.shard_map(
        body,
        mesh=mesh,
        in_specs=placed,
        out_specs=(P(("seq", "tp"), None), P("seq", "tp")),
        check_vma=False,
    )
```

```python
import functools
import math

import jax
import jax.numpy as jnp
from jax import lax
from jax.experimental import pallas as pl
from jax.experimental.pallas import tpu as pltpu
from jax.sharding import PartitionSpec as P

CH = 128
PAD = 8
VMEM_LIMIT = 66 * 1000 * 1000
F32, BF16 = jnp.float32, jnp.bfloat16


def mm(left, right, dims):
    return lax.dot_general(left, right, (dims, ((), ())), preferred_element_type=F32)


NN = ((1,), (0,))
NT = ((1,), (1,))
TN = ((0,), (0,))


def tri_sum(triangle, rows):
    high = rows.astype(BF16)
    low = (rows - high.astype(F32)).astype(BF16)
    return mm(triangle, high, NN) + mm(triangle, low, NN)


def kernel(
    seq, tp, dk, dv, tile, scale,
    tok, wq, wk, wv, wg, rate_ref, dout_ref,
    grad_ref, sig_ref,
    wcat, xbuf, proj, sq_all, w_all, s_all, m_all, cl_all, msg, got, edge,
    wout0, wout1, wout2, wout3, land0, land1, land2, land3, wfar, g_own, g_send, g_recv, part_own, part_send, part_recv,
    w_sem, x_sem, msg_send, msg_recv, gs_sem, gr_sem, ps_sem, pr_sem, first_sem, ring_s, ring_r,
):
    me, rank = lax.axis_index("seq"), lax.axis_index("tp")
    length, width = dout_ref.shape[0], wcat.shape[0]
    blocks, tiles = length // CH, length // tile
    each = blocks // tp
    half = each // 2
    core = rank + 1 - 2 * lax.rem(rank, 2)
    far = lax.rem(rank + 2, 4)
    far_core = lax.rem(core + 2, 4)
    half_ring, row = seq // 2, me // 2
    place = row + lax.rem(me, 2) * (seq - 1 - 2 * row)
    depth = width // seq

    def seq_at(p):
        p = lax.rem(p + seq, seq)
        return 2 * p + (p // half_ring) * (2 * seq - 1 - 4 * p)

    onward = (seq_at(place + 1), seq_at(place - 1))
    wouts, lands = (wout0, wout1, wout2, wout3), (land0, land1, land2, land3)
    starts = [sum(w.shape[0] for w in wouts[:n]) for n in range(4)]

    def cross(way):
        return pltpu.make_async_remote_copy(
            src_ref=wouts[way], dst_ref=lands[way].at[0], send_sem=first_sem.at[way],
            recv_sem=ring_r.at[way, 0], device_id={"tp": far},
            device_id_type=pl.DeviceIdType.MESH,
        )

    def ring(way, k):
        return pltpu.make_async_remote_copy(
            src_ref=lands[way].at[k], dst_ref=lands[way].at[k + 1], send_sem=ring_s.at[way, k],
            recv_sem=ring_r.at[way, k + 1], device_id={"seq": onward[way % 2]},
            device_id_type=pl.DeviceIdType.MESH,
        )

    def pump(k, part):
        for way in (2 * part, 2 * part + 1):
            if isinstance(k, int) and k == 0:
                cross(way).wait_recv()
            else:
                ring(way, k - 1).wait_recv()
            ring(way, k).start()

    def x_copy(t, slot):
        return pltpu.make_async_copy(
            tok.at[pl.ds(pl.multiple_of(t * tile, tile), tile), :], xbuf.at[slot], x_sem.at[slot]
        )

    loads = []
    for n, (w, start, size) in enumerate(
        ((wq, 0, dk), (wk, dk, dk), (wv, 2 * dk, dv), (wg, 2 * dk + dv, dk))
    ):
        loads.append(pltpu.make_async_copy(w, wcat.at[:, pl.ds(start, size)], w_sem.at[n]))
    x_copy(0, 0).start()
    for load in loads:
        load.start()

    barrier = pltpu.get_barrier_semaphore()
    for d in range(1, seq):
        pl.semaphore_signal(
            barrier, inc=1, device_id={"seq": lax.rem(me + d, seq)},
            device_id_type=pl.DeviceIdType.MESH,
        )
    for other in (core, far):
        pl.semaphore_signal(
            barrier, inc=1, device_id={"tp": other}, device_id_type=pl.DeviceIdType.MESH
        )

    rows_at = lax.broadcasted_iota(jnp.int32, (CH, CH), 0)
    cols_at = lax.broadcasted_iota(jnp.int32, (CH, CH), 1)
    lower = (rows_at >= cols_at).astype(F32)
    lower_b = lower.astype(BF16)
    upper_b = (rows_at <= cols_at).astype(BF16)
    rate = rate_ref[...]

    zero_state = jnp.zeros((dv, dk), F32)
    msg[0, pl.ds(0, dv), :] = zero_state
    msg[1, pl.ds(0, dv), :] = zero_state
    for load in loads:
        load.wait()
    for way in range(4):
        size = wouts[way].shape[0]
        at = pl.multiple_of(me * depth + starts[way], 16)
        wouts[way][...] = wcat[pl.ds(at, size), :].astype(F32)
    pl.semaphore_wait(barrier, seq + 1)
    for way in range(4):
        cross(way).start()

    def project(t, total):
        slot = lax.rem(t, 2)

        @pl.when(t + 1 < tiles)
        def _():
            x_copy(t + 1, 1 - slot).start()

        @pl.when(t == tiles - 2)
        def _():
            pump(0, 0)

        x_copy(t, slot).wait()
        out = mm(xbuf[slot], wcat[...], NN)
        base = pl.multiple_of(t * tile, tile)
        proj[pl.ds(base, tile), :] = out[:, : 2 * dk + dv].astype(BF16)
        squashed = jax.nn.sigmoid(out[:, 2 * dk + dv :])
        sq_all[pl.ds(base, tile), :] = squashed
        for j in range(tile // CH):
            part = slice(j * CH, (j + 1) * CH)
            b = t * (tile // CH) + j
            within = tri_sum(lower_b, -rate * squashed[part])
            w_all[pl.ds(pl.multiple_of(base + j * CH, CH), CH), :] = within
            closing = within[CH - 1 : CH]
            cl_all[b] = jnp.broadcast_to(closing, (PAD, dk))
            query = out[part, :dk].astype(BF16).astype(F32)
            key = out[part, dk : 2 * dk].astype(BF16).astype(F32)
            value = out[part, 2 * dk : 2 * dk + dv].astype(BF16)
            dout = dout_ref[pl.ds(pl.multiple_of(base + j * CH, CH), CH), :]
            query_scaled = (query * jnp.exp(within)).astype(BF16)
            key_closing = (key * jnp.exp(closing - within)).astype(BF16)
            state = msg[0, pl.ds(0, dv), :]
            s_all[b] = state
            msg[0, pl.ds(0, dv), :] = jnp.exp(closing) * state + mm(value, key_closing, TN)
            fed = mm(dout, query_scaled, TN)
            m_all[b] = fed
            msg[1, pl.ds(0, dv), :] += jnp.exp(total) * fed
            total = total + closing
        return total

    total = lax.fori_loop(0, tiles, project, jnp.zeros((1, dk), F32))
    decay = jnp.broadcast_to(jnp.exp(total), (PAD, dk))
    msg[0, pl.ds(dv, PAD), :] = decay
    msg[1, pl.ds(dv, PAD), :] = decay

    def exchange(d):
        return pltpu.make_async_remote_copy(
            src_ref=msg.at[(me + d) // seq],
            dst_ref=got.at[d],
            send_sem=msg_send.at[d],
            recv_sem=msg_recv.at[d],
            device_id={"seq": lax.rem(me + d, seq)},
            device_id_type=pl.DeviceIdType.MESH,
        )

    def start_exchange(d, carry):
        exchange(d).start()
        return carry

    def wait_exchange(d, carry):
        exchange(d).wait()
        return carry

    lax.fori_loop(1, seq, start_exchange, 0)
    pump(0, 1)
    lax.fori_loop(1, seq, wait_exchange, 0)

    edge[...] = jnp.zeros_like(edge)

    def fold(which, d):
        edge[which] = got[d, pl.ds(dv, 1), :] * edge[which] + got[d, pl.ds(0, dv), :]

    def fold_states(j, carry):
        fold(0, me - j)
        return carry

    def fold_grads(d, carry):
        fold(1, d)
        return carry

    lax.fori_loop(0, me, fold_states, 0)
    lax.fori_loop(me + 1, seq, fold_grads, 0)

    def enter(b, so_far):
        s_all[b] = s_all[b] + jnp.exp(so_far) * edge[0]
        return so_far + cl_all[b, 0:1, :]

    lax.fori_loop(0, blocks, enter, jnp.zeros((1, dk), F32))

    def leave(j, carry):
        b = blocks - 1 - j
        fed = m_all[b]
        leaving = edge[1]
        m_all[b] = leaving
        edge[1] = jnp.exp(cl_all[b, 0:1, :]) * leaving + fed
        return carry

    lax.fori_loop(0, blocks, leave, 0)

    def grads(b):
        rows = pl.ds(pl.multiple_of(b * CH, CH), CH)
        query = proj[rows, 0:dk].astype(F32)
        key = proj[rows, dk : 2 * dk].astype(F32)
        value = proj[rows, 2 * dk : 2 * dk + dv]
        within, squashed, dout = w_all[rows, :], sq_all[rows, :], dout_ref[rows, :]
        closing = within[CH - 1 : CH]
        state, leaving = s_all[b], m_all[b]
        grow, shrink, rest = jnp.exp(within), jnp.exp(-within), jnp.exp(closing - within)
        query_f, key_f, close_f = query * grow, key * shrink, key * rest
        query_s, key_s, close_s = query_f.astype(BF16), key_f.astype(BF16), close_f.astype(BF16)
        scores = (mm(query_s, key_s, NT) * lower).astype(BF16)
        d_scores = (mm(dout, value, NT) * lower).astype(BF16)
        leaving_b = leaving.astype(BF16)
        d_query_s = mm(dout, state.astype(BF16), NN) + mm(d_scores, key_s, NN)
        d_key_s = mm(d_scores, query_s, TN)
        d_close = mm(value, leaving_b, NN)
        d_value = mm(scores, dout, TN) + mm(close_s, leaving_b, NT)
        d_query = d_query_s * grow
        d_key = d_key_s * shrink + d_close * rest
        at_close = d_close * close_f
        d_within = d_query_s * query_f - d_key_s * key_f - at_close
        d_closing = jnp.sum(at_close, axis=0, keepdims=True) + jnp.exp(closing) * jnp.sum(
            leaving * state, axis=0, keepdims=True
        )
        d_gate = tri_sum(upper_b, d_within) + d_closing
        pre = d_gate * -rate * squashed * (1.0 - squashed)
        sig_ref[rows, :] = pre * scale
        return d_query, d_key, d_value, pre

    bounds = ((0, dk), (dk, 2 * dk), (2 * dk, 2 * dk + dv), (2 * dk + dv, 3 * dk + dv))
    step = 512 if width % 512 == 0 else width

    def spread(packed, weight, put):
        for at in range(0, width, step):
            cols = slice(at, at + step)
            put(cols, mm(packed, weight[cols, :], NT))

    def copy_g(i):
        return pltpu.make_async_remote_copy(
            src_ref=g_send.at[i], dst_ref=g_recv.at[i], send_sem=gs_sem.at[i],
            recv_sem=gr_sem.at[i], device_id={"tp": far}, device_id_type=pl.DeviceIdType.MESH,
        )

    def copy_p(i):
        return pltpu.make_async_remote_copy(
            src_ref=part_send.at[i], dst_ref=part_recv.at[i], send_sem=ps_sem.at[i],
            recv_sem=pr_sem.at[i], device_id={"tp": core}, device_id_type=pl.DeviceIdType.MESH,
        )

    steps = iter([(k, part) for k in range(1, seq - 1) for part in (0, 1)])

    def pump_next():
        k = next(steps, None)
        if k is not None:
            pump(*k)

    def away(chunk, base):
        def run(i, carry):
            for (lo, hi), part in zip(bounds, grads(chunk * each + i)):
                g_send[base + i, :, lo:hi] = part
            copy_g(base + i).start()
            return carry

        lax.fori_loop(0, half, run, 0)
        pump_next()
        lax.fori_loop(half, each, run, 0)
        pump_next()

    def home(chunk, base):
        def run(i, carry):
            for (lo, hi), part in zip(bounds, grads(chunk * each + i)):
                g_own[base + i, :, lo:hi] = part.astype(BF16)
            return carry

        lax.fori_loop(0, half, run, 0)
        pump_next()
        lax.fori_loop(half, each, run, 0)
        pump_next()

    def rows_of(buffer, i):
        return jnp.concatenate([buffer[2 * i], buffer[2 * i + 1]], axis=0).astype(BF16)

    away(far_core, 0)
    away(far, each)
    home(core, 0)
    home(rank, each)

    def own_part(i, carry):
        def put_send(cols, part):
            part_send[i, :, cols] = part

        def put_own(cols, part):
            part_own[i, :, cols] = part

        spread(rows_of(g_own, i), wcat, put_send)
        spread(rows_of(g_own, half + i), wcat, put_own)
        return carry

    lax.fori_loop(0, half, own_part, 0)
    done, part = next(steps, (seq - 1, 0))
    if part == 1:
        pump(done, 1)
        done += 1

    def pump_rest(k, carry):
        pump(k, 0)
        pump(k, 1)
        return carry

    lax.fori_loop(done, seq - 1, pump_rest, 0)
    for way in range(4):
        ring(way, seq - 2).wait_recv()

    def unpack(k, carry):
        for way in range(4):
            origin = seq_at(place + k) if way % 2 else seq_at(place - k)
            size = wouts[way].shape[0]
            at = pl.multiple_of(origin * depth + starts[way], 16)
            wfar[pl.ds(at, size), :] = lands[way][k].astype(BF16)
        return carry

    lax.fori_loop(0, seq, unpack, 0)

    def send_part(i, carry):
        copy_g(2 * i).wait()
        copy_g(2 * i + 1).wait()

        def put(cols, part):
            part_send[i, :, cols] = part_send[i, :, cols] + part

        spread(rows_of(g_recv, i), wfar, put)
        copy_p(i).start()
        return carry

    lax.fori_loop(0, half, send_part, 0)

    def finish(i, carry):
        copy_g(2 * (half + i)).wait()
        copy_g(2 * (half + i) + 1).wait()
        copy_p(i).wait()
        rows = pl.ds(pl.multiple_of(i * 2 * CH, 2 * CH), 2 * CH)

        def put(cols, part):
            grad_ref[rows, cols] = (
                part_own[i, :, cols] + part + part_recv[i, :, cols]
            ).astype(BF16)

        spread(rows_of(g_recv, half + i), wfar, put)
        return carry

    lax.fori_loop(0, half, finish, 0)

    def drain(k, carry):
        for way in range(4):
            ring(way, k).wait_send()
        return carry

    for way in range(4):
        cross(way).wait_send()
    lax.fori_loop(0, seq - 1, drain, 0)


def solution(mesh):
    seq, tp = mesh.shape["seq"], mesh.shape["tp"]

    def body(tokens, w_query, w_key, w_value, w_gate, gate_rate, out_grad):
        length, width = tokens.shape
        dk, dv = w_query.shape[1], w_value.shape[1]
        blocks, each = length // CH, length // CH // tp
        tile = 2 * CH
        scale = 4.0 * math.sqrt(length * seq * dk / dv)
        depth = width // seq
        units = depth // 16
        sizes = [16 * ((units + 3 - n) // 4) for n in range(4)]
        hbm = pl.BlockSpec(memory_space=pl.ANY)
        vmem = pl.BlockSpec(memory_space=pltpu.VMEM)
        dma = pltpu.SemaphoreType.DMA
        return pl.pallas_call(
            functools.partial(kernel, seq, tp, dk, dv, tile, scale),
            out_shape=(
                jax.ShapeDtypeStruct((length // tp, width), BF16),
                jax.ShapeDtypeStruct((length, dk), F32),
            ),
            in_specs=[hbm] * 5 + [vmem] * 2,
            out_specs=(vmem, vmem),
            scratch_shapes=[
                pltpu.VMEM((width, 3 * dk + dv), BF16),
                pltpu.VMEM((2, tile, width), BF16),
                pltpu.VMEM((length, 2 * dk + dv), BF16),
                pltpu.VMEM((length, dk), F32),
                pltpu.VMEM((length, dk), F32),
                pltpu.VMEM((blocks, dv, dk), F32),
                pltpu.VMEM((blocks, dv, dk), F32),
                pltpu.VMEM((blocks, PAD, dk), F32),
                pltpu.VMEM((2, dv + PAD, dk), F32),
                pltpu.VMEM((seq, dv + PAD, dk), F32),
                pltpu.VMEM((2, dv, dk), F32),
            ]
            + [pltpu.VMEM((size, 3 * dk + dv), F32) for size in sizes]
            + [pltpu.VMEM((seq, size, 3 * dk + dv), F32) for size in sizes]
            + [pltpu.VMEM((width, 3 * dk + dv), BF16)]
            + [pltpu.VMEM((2 * each, CH, 3 * dk + dv), kind) for kind in (BF16, F32, F32)]
            + [pltpu.VMEM((each // 2, 2 * CH, width), F32)] * 3
            + [dma((4,)), dma((2,)), dma((seq,)), dma((seq,))]
            + [dma((2 * each,))] * 2
            + [dma((each // 2,))] * 2
            + [dma((4,)), dma((4, seq)), dma((4, seq))],
            compiler_params=pltpu.CompilerParams(
                collective_id=0, has_side_effects=True, vmem_limit_bytes=VMEM_LIMIT
            ),
        )(tokens, w_query, w_key, w_value, w_gate, gate_rate.reshape(1, dk), out_grad)

    placed = (
        P("seq", None),
        P(None, "tp"),
        P(None, "tp"),
        P(None, "tp"),
        P(None, "tp"),
        P("tp"),
        P("seq", "tp"),
    )
    return jax.shard_map(
        body,
        mesh=mesh,
        in_specs=placed,
        out_specs=(P(("seq", "tp"), None), P("seq", "tp")),
        check_vma=False,
    )
```
